128 devices in a mesh: ta: 2 (over core), ha: 2 (over z_hi), wa: 32 (over z_lo, x, y).
Axes of the slice: x: 4, y: 4, z: 4 (z_hi: 2, z_lo: 2; z = z_hi * 2 + z_lo), core: 2. Of those that a mesh axis runs over, the one named last changes fastest.
Arguments:
- features: bfloat16 [2, 16, 28, 448, 1024], P(None, 'ta', 'ha', 'wa'), may hold values from -6 to 6
- teacher: bfloat16 [2, 16, 28, 448, 1000], P(None, 'ta', 'ha', 'wa'), may hold values from -30 to 750
- head_weight: float32 [1024, 1000], replicated, may hold values from -0.1875 to 0.1875
Outputs:
- feature_grad: bfloat16 [2, 16, 28, 448, 1024], P(None, 'ta', 'ha', 'wa')
- loss: float32 [], replicated
- new_weight: float32 [1024, 1000], P(('ta', 'ha', 'wa'))
The draws below stay inside these ranges and needn't reach their ends.
All inputs are finite; a program needn't handle non-finite values.
Results may differ from the reference program's by a relative error of at most 0.0056.
Values may be sent and summed in bfloat16 or wider, within the bound.
No kernel may reach another device: no remote copies, remote signals or barrier semaphores. Data moves between devices by JAX's collectives and lax.ppermute only.
A program may use at most 192 MiB of HBM per device.

```python
import jax
import jax.numpy as jnp
from jax import lax

D = 1024
CLASSES = 1000
BATCH = 2
WW = 14
WV = 28
NT = 16
NH = 28
NW = 448


def draw_teacher(key, part):
    key_noise = jax.random.fold_in(jax.random.fold_in(key, 17), 0)
    shape = (BATCH, NT, NH, NW, CLASSES)
    return jnp.clip(3.0 * jax.random.normal(key_noise, shape, jnp.float32), -18.0, 18.0).astype(jnp.bfloat16)


def strengthened(array, own_key, source, target, parts, factor):
    owner, partner = [(jnp.arange(array.shape[axis_at]) // (array.shape[axis_at] // parts)).reshape([-1 if axis == axis_at else 1 for axis in range(array.ndim)]) for axis_at in (source, target)]
    chosen = jax.random.permutation(own_key, parts)[partner]
    strong = (owner == chosen) | (owner == (partner + parts // 2) % parts)
    return jnp.where(strong, factor * array, array)


def shard_levels(stream_key, extent, shards, least, top_value):
    loudness = 1.0
    for position, blocks in shards:
        draws = jax.random.uniform(jax.random.fold_in(jax.random.fold_in(stream_key, 6), position), (blocks,), jnp.float32, least / len(shards), top_value / len(shards))
        loudness = loudness * jnp.repeat(jnp.exp(draws), extent[position] // blocks).reshape((-1,) + (1,) * (len(extent) - 1 - position))
    return loudness


def centred(key, extent, spread, bound, shards=(), kind=jnp.bfloat16):
    factor_of = shard_levels(key, extent, shards, -0.22, 0.18) if shards else 1.0
    array = jax.random.normal(key, extent, jnp.float32) * spread * factor_of
    return jnp.minimum(jnp.maximum(array, -bound), bound).astype(kind)


def bell_draw_with(stream_key, dims, deviation, limit, pieces, heavy, kind=jnp.bfloat16):
    values = deviation * jax.random.normal(stream_key, dims, jnp.float32)
    if pieces:
        values = values * shard_levels(stream_key, dims, pieces, -0.22, 0.18)
    return jnp.clip(strengthened(values, jax.random.fold_in(stream_key, 3), *heavy), -limit, limit).astype(kind)


def setup_inputs(seed: int = 0) -> dict:
    keys = jax.random.split(jax.random.key(seed), 4)
    return {
        "features": bell_draw_with(keys[0], (BATCH, NT, NH, NW, D), 1.0, 6.0, ((1, 2), (2, 2), (3, 32)), (3, 4, 32, 2.75)),
        "teacher": draw_teacher(jax.random.fold_in(keys[3], 71), 0),
        "head_weight": centred(keys[2], (D, CLASSES), D ** -0.5, 0.1875, (), jnp.float32),
    }


sharpness_divisor = 2.0
learn_rate = 0.1
clip_norm = 1000.0

def pool_axis(values, reduce_dimension):
    width = [(0, 0)] * values.ndim
    width[reduce_dimension] = (1, 1)
    padded = jnp.pad(values, width)
    length = values.shape[reduce_dimension]
    first = lax.slice_in_dim(padded, 0, length, axis=reduce_dimension)
    middle = lax.slice_in_dim(padded, 1, length + 1, axis=reduce_dimension)
    last = lax.slice_in_dim(padded, 2, length + 2, axis=reduce_dimension)
    return first + middle + last

def clip_of(columns):
    return (columns + WV - WW // 2) // WV

def reference(features, teacher, head_weight):
    head_bf = head_weight.astype(jnp.bfloat16)
    blocks_wide = NW // WV
    teacher_padded = jnp.pad(teacher, ((0, 0), (0, 0), (0, 0), (1, 1), (0, 0)))
    frame_ids = jnp.arange(NT, dtype=jnp.int32)
    row_ids = jnp.arange(NH, dtype=jnp.int32)
    frame_count = (3.0 - (frame_ids == 0).astype(jnp.float32) - (frame_ids == NT - 1).astype(jnp.float32)).reshape(1, NT, 1, 1, 1)
    row_count = (3.0 - (row_ids == 0).astype(jnp.float32) - (row_ids == NH - 1).astype(jnp.float32)).reshape(1, 1, NH, 1, 1)

    def one_block(carry, block):
        head_grad, overall_objective, output = carry
        start = (block * WV).astype(jnp.int32)
        feat_block = lax.dynamic_slice_in_dim(features, start, WV, 3)
        teach_block = lax.dynamic_slice_in_dim(teacher_padded, start, WV + 2, 3).astype(jnp.float32)
        columns = start + jnp.arange(WV, dtype=jnp.int32)
        own_clip = clip_of(columns)
        left_ok = ((columns > 0) & (clip_of(columns - 1) == own_clip)).astype(jnp.float32).reshape(1, 1, 1, WV, 1)
        right_ok = ((columns < NW - 1) & (clip_of(columns + 1) == own_clip)).astype(jnp.float32).reshape(1, 1, 1, WV, 1)
        planar = pool_axis(pool_axis(teach_block, 1), 2)
        summed = planar[:, :, :, 0:WV] * left_ok + planar[:, :, :, 1:WV + 1] + planar[:, :, :, 2:WV + 2] * right_ok
        counts = frame_count * row_count * (1.0 + left_ok + right_ok)
        averaged_scores = (summed / counts).reshape(-1, CLASSES)
        feat_rows = feat_block.reshape(-1, D)
        pupil_scores = jnp.dot(feat_rows, head_bf, preferred_element_type=jnp.float32)
        pupil_entropy_terms = jax.nn.log_softmax(pupil_scores / sharpness_divisor, axis=-1)
        mentor_entropy_terms = jax.nn.log_softmax(averaged_scores / sharpness_divisor, axis=-1)
        mentor_likelihoods = jnp.exp(mentor_entropy_terms)
        pupil_likelihoods = jnp.exp(pupil_entropy_terms)
        patch_kullback_leibler = lax.optimization_barrier(jnp.sum(mentor_likelihoods * (mentor_entropy_terms - pupil_entropy_terms), axis=-1))
        overall_objective = overall_objective + sharpness_divisor * sharpness_divisor * jnp.sum(patch_kullback_leibler)
        score_slope = (sharpness_divisor * (pupil_likelihoods - mentor_likelihoods)).astype(jnp.bfloat16)
        feat_grad = lax.dot_general(score_slope, head_bf, (((1,), (1,)), ((), ())), preferred_element_type=jnp.float32)
        feat_grad = feat_grad.astype(jnp.bfloat16).reshape(feat_block.shape)
        output = lax.dynamic_update_slice_in_dim(output, feat_grad, start, 3)
        head_grad = head_grad + lax.dot_general(feat_rows, score_slope, (((0,), (0,)), ((), ())), preferred_element_type=jnp.float32)
        return ((head_grad, overall_objective, output), None)
    start_carry = (jnp.zeros((D, CLASSES), jnp.float32), jnp.zeros((), jnp.float32), jnp.zeros(features.shape, jnp.bfloat16))
    (head_grad, loss, feature_grad), _ = lax.scan(one_block, start_carry, jnp.arange(blocks_wide, dtype=jnp.int32))
    grad_norm = jnp.sqrt(jnp.sum(head_grad * head_grad))
    clip = jnp.minimum(1.0, clip_norm / (grad_norm + 1e-06))
    new_weight = head_weight - learn_rate * clip * head_grad
    return (feature_grad, loss, new_weight)
```

```python
import functools

import jax
import jax.numpy as jnp
import numpy as np
from jax import lax
from jax.experimental import pallas as pl
from jax.experimental.pallas import tpu as pltpu
from jax.sharding import PartitionSpec as P

WW = 14
WV = 28
LR = 0.1
CLIP = 1000.0
LOG2E = 1.4426950408889634
LN2 = 0.6931471805599453
AXES = ("ta", "ha", "wa")
SWAP = [(0, 1), (1, 0)]


def clip_of(columns):
    return (columns + WV - WW // 2) // WV


def prep_kernel(rows, cols, steps, sel_ref, x_ref, out_ref, edge):
    step = pl.program_id(0)
    width = cols * 8
    for s in range(steps):

        @pl.when(step == s)
        def _(s=s):
            for i in range(rows):
                n = s * rows + i
                tile = jnp.dot(
                    sel_ref[...], x_ref[i * width : (i + 1) * width, :], preferred_element_type=jnp.float32
                )
                out_ref[n * 16 : (n + 1) * 16, :] = tile.astype(jnp.bfloat16)
                edge[n : n + 1, :] = tile[cols - 1 : cols]
                edge[32 + n : 33 + n, :] = tile[0:1]

    @pl.when(step == steps - 1)
    def _():
        total = steps * rows
        out_ref[total * 16 : total * 16 + 64, :] = edge[...].astype(jnp.bfloat16)


def student_kernel(chunk, f_ref, w_ref, zs_ref, s_ref):
    s_ref[...] = lax.dot_general(
        f_ref[...], w_ref[...], (((1,), (1,)), ((), ())), preferred_element_type=jnp.float32
    )

    def body(i, carry):
        at = pl.ds(pl.multiple_of(i * chunk, chunk), chunk)
        s = s_ref[at, :]
        z = (s - jnp.max(s, axis=1, keepdims=True)) * (0.5 * LOG2E)
        total = jnp.sum(jnp.exp2(z), axis=1, keepdims=True)
        zs_ref[at, :] = z - (jnp.log2(total) - 1.0)
        return carry

    lax.fori_loop(0, s_ref.shape[0] // chunk, body, 0)


def teacher_kernel(
    grid_h, rows, span, ha_ref, a_ref, x_ref, ext_ref, hm_ref, hx_ref, cw_ref, zs_ref, out_ref, kl_ref, sums
):
    half = pl.program_id(1)
    ha = ha_ref[0]
    per = rows // span
    a = a_ref[...]

    def pool(x, y):
        return jnp.dot(a, jnp.concatenate([x, y], axis=0), preferred_element_type=jnp.float32)

    def local(i):
        r = half * per - 1 + i
        x = x_ref[pl.ds(pl.multiple_of(r * 112, 16), 112), :]
        y = ext_ref[pl.ds(pl.multiple_of(r * 32, 16), 32), :]
        sums[i] = pool(x, y)

    for i in range(1, per + 1):
        local(i)
    for i, side, here in ((0, half == 0, ha == 1), (per + 1, half == span - 1, ha == 0)):

        @pl.when(jnp.logical_not(side))
        def _(i=i):
            local(i)

        @pl.when(jnp.logical_and(side, here))
        def _(i=i):
            sums[i] = pool(hm_ref[...], hx_ref[...])

        @pl.when(jnp.logical_and(side, jnp.logical_not(here)))
        def _(i=i):
            sums[i] = jnp.zeros(sums.shape[1:], jnp.float32)

    @pl.when(jnp.logical_and(pl.program_id(0) == 0, half == 0))
    def _():
        kl_ref[...] = jnp.zeros_like(kl_ref)

    def body(k, carry):
        at = pl.ds(pl.multiple_of(k * 112, 16), 112)
        row = ha * rows + half * per + k
        edge = jnp.logical_or(row == 0, row == grid_h - 1)
        scale = cw_ref[...] * jnp.where(edge, 1.0 / 2.0, 1.0 / 3.0)
        z = (sums[k] + sums[k + 1] + sums[k + 2]) * scale[:, 0:1]
        z = z - jnp.max(z, axis=1, keepdims=True)
        e = jnp.exp2(z)
        zs = zs_ref[at, :]
        total = jnp.sum(e, axis=1, keepdims=True)
        cross = jnp.sum(e * (z - zs), axis=1, keepdims=True)
        inv = 1.0 / total
        out_ref[at, :] = (jnp.exp2(zs) - e * (2.0 * inv)).astype(jnp.bfloat16)
        kl_ref[...] += jnp.broadcast_to(cross * inv - jnp.log2(total) + 1.0, kl_ref.shape)
        return carry

    lax.fori_loop(0, per, body, 0)


def local(features, teacher, head_weight):
    batch, frames, rows, columns, width = features.shape
    classes = teacher.shape[-1]
    n_wa = lax.axis_size("wa")
    grid_w = columns * n_wa
    grid_h = rows * lax.axis_size("ha")
    grid_t = frames * lax.axis_size("ta")
    ta, ha, wa = (lax.axis_index(name) for name in AXES)
    tokens = batch * rows * columns * frames
    group = columns * frames
    forward = [(i, i + 1) for i in range(n_wa - 1)]
    backward = [(i + 1, i) for i in range(n_wa - 1)]

    feat = features.transpose(0, 2, 3, 1, 4).reshape(tokens, width)
    teach5 = teacher.transpose(0, 2, 3, 1, 4)
    teach = teach5.reshape(tokens, classes)
    wt = head_weight.T
    wt_bf = wt.astype(jnp.bfloat16)

    edge_t = jnp.where(ta == 0, frames - 1, 0)
    pick = np.arange(16)[:, None] * frames
    sel = (jnp.arange(group)[None, :] == pick + edge_t).astype(jnp.bfloat16)

    k = np.arange(144)
    kw = np.where(k < 112, k // 8, np.where(k < 120, -1, np.where(k < 128, 14, k - 128)))
    kw = np.where(k == 142, -1, np.where(k == 143, 14, kw))
    kt = np.where(k < 112, k % 8, np.where(k < 128, (k - 112) % 8, 0))
    halo = k >= 128
    kt = jnp.where(halo, jnp.where(ta == 0, frames, -1), kt)[None, :]
    kw = kw[None, :]
    w = (np.arange(group) // frames)[:, None]
    t = (np.arange(group) % frames)[:, None]
    col, kcol = wa * columns + w, wa * columns + kw
    near = (abs(w - kw) <= 1) & (abs(t - kt) <= 1)
    ok = (kcol >= 0) & (kcol < grid_w) & (clip_of(kcol) == clip_of(col))
    pool = (near & ok).astype(jnp.bfloat16)
    left_ok = (col > 0) & (clip_of(col - 1) == clip_of(col))
    right_ok = (col < grid_w - 1) & (clip_of(col + 1) == clip_of(col))
    frame = ta * frames + t
    count = (3.0 - (frame == 0) - (frame == grid_t - 1)) * (1.0 + left_ok + right_ok)
    scale = jnp.broadcast_to((0.5 * LOG2E) / count.astype(jnp.float32), (group, 128))

    h_edge = jnp.where(ha == 0, rows - 1, 0)
    left = lax.ppermute(teach5[:, :, columns - 1], "wa", forward)
    right = lax.ppermute(teach5[:, :, 0], "wa", backward)
    h_main = lax.ppermute(lax.dynamic_index_in_dim(teach5, h_edge, 1, False), "ha", SWAP)
    steps = 4
    per = batch * rows // steps
    face = pl.pallas_call(
        functools.partial(prep_kernel, per, columns, steps),
        grid=(steps,),
        in_specs=[
            pl.BlockSpec((16, group), lambda i: (0, 0)),
            pl.BlockSpec((per * group, classes), lambda i: (i, 0)),
        ],
        out_specs=pl.BlockSpec((batch * rows * 16 + 64, classes), lambda i: (0, 0)),
        out_shape=jax.ShapeDtypeStruct((batch * rows * 16 + 64, classes), jnp.bfloat16),
        scratch_shapes=[pltpu.VMEM((64, classes), jnp.float32)],
        cost_estimate=pl.CostEstimate(flops=10**9, bytes_accessed=8 * 10**6, transcendentals=0),
    )(sel, teach)
    face = lax.ppermute(face, "ta", SWAP)
    n = batch * rows * 16
    corner_l = lax.ppermute(face[n : n + 32], "wa", forward)
    corner_r = lax.ppermute(face[n + 32 : n + 64], "wa", backward)
    ext = jnp.concatenate(
        [
            left,
            right,
            face[:n].reshape(batch, rows, 16, classes)[:, :, :columns],
            corner_l[: batch * rows].reshape(batch, rows, 1, classes),
            corner_r[: batch * rows].reshape(batch, rows, 1, classes),
        ],
        axis=2,
    )
    h_ext = lax.ppermute(lax.dynamic_index_in_dim(ext, h_edge, 1, False), "ha", SWAP)

    block = 448
    zs = pl.pallas_call(
        functools.partial(student_kernel, 112),
        grid=(tokens // block,),
        in_specs=[
            pl.BlockSpec((block, width), lambda i: (i, 0)),
            pl.BlockSpec((classes, width), lambda i: (0, 0)),
        ],
        out_specs=pl.BlockSpec((block, classes), lambda i: (i, 0)),
        out_shape=jax.ShapeDtypeStruct((tokens, classes), jnp.float32),
        scratch_shapes=[pltpu.VMEM((block, classes), jnp.float32)],
        cost_estimate=pl.CostEstimate(
            flops=2 * tokens * width * classes, bytes_accessed=22 * 10**6, transcendentals=tokens * classes
        ),
    )(feat, wt_bf)

    span = 2
    big = rows // span * group
    slope, kl = pl.pallas_call(
        functools.partial(teacher_kernel, grid_h, rows, span),
        grid=(batch, span),
        in_specs=[
            pl.BlockSpec(memory_space=pltpu.SMEM),
            pl.BlockSpec((group, 144), lambda b, s: (0, 0)),
            pl.BlockSpec((rows * group, classes), lambda b, s: (b, 0)),
            pl.BlockSpec((rows * 32, classes), lambda b, s: (b, 0)),
            pl.BlockSpec((group, classes), lambda b, s: (b, 0)),
            pl.BlockSpec((32, classes), lambda b, s: (b, 0)),
            pl.BlockSpec((group, 128), lambda b, s: (0, 0)),
            pl.BlockSpec((big, classes), lambda b, s: (b * span + s, 0)),
        ],
        out_specs=[
            pl.BlockSpec((big, classes), lambda b, s: (b * span + s, 0)),
            pl.BlockSpec((group, 128), lambda b, s: (0, 0)),
        ],
        out_shape=[
            jax.ShapeDtypeStruct((tokens, classes), jnp.bfloat16),
            jax.ShapeDtypeStruct((group, 128), jnp.float32),
        ],
        scratch_shapes=[pltpu.VMEM((rows // span + 2, group, classes), jnp.float32)],
        compiler_params=pltpu.CompilerParams(vmem_limit_bytes=48 * 2**20),
        cost_estimate=pl.CostEstimate(
            flops=4 * 10**9, bytes_accessed=27 * 10**6, transcendentals=2 * tokens * classes
        ),
    )(
        ha.astype(jnp.int32).reshape(1),
        pool,
        teach,
        ext.reshape(batch * rows * 32, classes),
        h_main.reshape(batch * group, classes),
        h_ext.reshape(batch * 32, classes),
        scale,
        zs,
    )

    n_dev = lax.axis_size(AXES)
    owned = width // n_dev
    head_part = lax.dot_general(feat, slope, (((0,), (0,)), ((), ())), preferred_element_type=jnp.float32)
    pieces = lax.all_to_all(
        head_part.astype(jnp.bfloat16).reshape(n_dev, owned, classes), AXES, 0, 0, tiled=True
    )
    feat_grad = jnp.dot(slope, wt_bf, preferred_element_type=jnp.float32).astype(jnp.bfloat16)
    feature_grad = feat_grad.reshape(batch, rows, columns, frames, width).transpose(0, 3, 1, 2, 4)

    mine = jnp.sum(pieces.astype(jnp.float32), axis=0)
    pair = jnp.stack([jnp.sum(mine * mine), jnp.sum(kl[:, 0])])
    pair = jnp.pad(pair, (0, 126)).reshape(1, 1, 128)
    pair = lax.all_to_all(jnp.broadcast_to(pair, (n_dev, 1, 128)), AXES, 0, 0, tiled=True)
    pair = jnp.sum(pair, axis=(0, 1))
    loss = pair[1] * (4.0 * LN2)
    clip = jnp.minimum(1.0, CLIP / (jnp.sqrt(pair[0]) + 1e-06))
    first = lax.axis_index(AXES) * owned
    weight_rows = lax.dynamic_slice_in_dim(head_weight, first, owned, 0)
    new_weight = weight_rows - LR * clip * mine
    return feature_grad, loss, new_weight


def solution(mesh):
    placed = P(None, "ta", "ha", "wa", None)
    return jax.shard_map(
        local,
        mesh=mesh,
        in_specs=(placed, placed, P()),
        out_specs=(placed, P(), P(AXES, None)),
        check_vma=False,
    )
```

```python
import functools

import jax
import jax.numpy as jnp
import numpy as np
from jax import lax
from jax.experimental import pallas as pl
from jax.experimental.pallas import tpu as pltpu
from jax.sharding import PartitionSpec as P

WW = 14
WV = 28
LR = 0.1
CLIP = 1000.0
LOG2E = 1.4426950408889634
LN2 = 0.6931471805599453
AXES = ("ta", "ha", "wa")
SWAP = [(0, 1), (1, 0)]
F32 = jnp.float32
BF16 = jnp.bfloat16


def clip_of(columns):
    return (columns + WV - WW // 2) // WV


def cost(flops, moved, trans=0):
    return pl.CostEstimate(flops=int(flops), bytes_accessed=int(moved), transcendentals=int(trans))


def params():
    return pltpu.CompilerParams(vmem_limit_bytes=60 * 1024 * 1024)


def prep_kernel(
    rows, cols, steps, batch, h_ref, sel_ref, x_ref, c0_ref, c1_ref, hr_ref,
    first_ref, last_ref, row_ref, face_ref, e0_ref, e1_ref, s0, s1
):
    step = pl.program_id(0)
    per = rows * batch // steps
    width = cols * 8

    @pl.when(step == 0)
    def _():
        first_ref[...] = c0_ref[...].reshape(first_ref.shape)
        last_ref[...] = c1_ref[...].reshape(last_ref.shape)
        row_ref[...] = hr_ref[...].reshape(row_ref.shape)
        s0[...] = jnp.zeros_like(s0)
        s1[...] = jnp.zeros_like(s1)

    for s in range(steps):

        @pl.when(step == s)
        def _(s=s):
            for i in range(per):
                b, h = divmod(s * per + i, rows)
                tile = jnp.dot(
                    sel_ref[...], x_ref[i * width : (i + 1) * width, :], preferred_element_type=F32
                )
                face_ref[(b * rows + h) * 16 : (b * rows + h + 1) * 16, :] = tile.astype(BF16)
                s0[b * 16 + h : b * 16 + h + 1, :] = tile[0:1]
                s1[b * 16 + h : b * 16 + h + 1, :] = tile[cols - 1 : cols]

    @pl.when(step == steps - 1)
    def _():
        e0_ref[...] = s0[...].astype(BF16)
        e1_ref[...] = s1[...].astype(BF16)


def beside(left, right):
    return jnp.concatenate([left.astype(F32), right.astype(F32)], axis=0).astype(BF16)


def with_corners(face, low, high):
    row = lax.broadcasted_iota(jnp.int32, face.shape, 0)
    tile = jnp.where(row == 14, low, face.astype(F32))
    return jnp.where(row == 15, high, tile).astype(BF16)


def pack_kernel(batch, h_ref, l_ref, r_ref, f_ref, el_ref, er_ref, out_ref):
    h = h_ref[0]
    for b in range(batch):
        out_ref[b, 0:16, :] = beside(l_ref[b, 0], r_ref[b, 0])
        row = lax.broadcasted_iota(jnp.int32, el_ref.shape[1:], 0)
        low = jnp.sum(jnp.where(row == h, el_ref[b].astype(F32), 0.0), axis=0, keepdims=True)
        high = jnp.sum(jnp.where(row == h, er_ref[b].astype(F32), 0.0), axis=0, keepdims=True)
        out_ref[b, 16:32, :] = with_corners(f_ref[b, 0], low, high)


def student_rows(s_ref, zs_ref, chunk):
    for i in range(s_ref.shape[0] // chunk):
        at = slice(i * chunk, (i + 1) * chunk)
        s = s_ref[at, :]
        z = (s - jnp.max(s, axis=1, keepdims=True)) * (0.5 * LOG2E)
        total = jnp.sum(jnp.exp2(z), axis=1, keepdims=True)
        zs_ref[at, :] = z - (jnp.log2(total) - 1.0)


def student_kernel(blocks, convert, f_ref, w_ref, *rest):
    if convert:
        zs_ref, w_bf, even, odd = rest
    else:
        w_bf, (_, zs_ref, even, odd) = w_ref, rest
    step = pl.program_id(0)

    if convert:

        @pl.when(step == 0)
        def _():
            w_bf[...] = w_ref[...].astype(BF16)

    def matmul(to):
        to[...] = lax.dot_general(
            f_ref[...], w_bf[...], (((1,), (1,)), ((), ())), preferred_element_type=F32
        )

    @pl.when(step == 0)
    def _():
        matmul(even)

    middle = jnp.logical_and(step > 0, step < blocks)

    @pl.when(jnp.logical_and(middle, step % 2 == 1))
    def _():
        matmul(odd)
        student_rows(even, zs_ref, 16)

    @pl.when(jnp.logical_and(middle, step % 2 == 0))
    def _():
        matmul(even)
        student_rows(odd, zs_ref, 16)

    @pl.when(step == blocks)
    def _():
        student_rows(even if blocks % 2 == 1 else odd, zs_ref, 16)


def teacher_kernel(
    grid_h, rows, span, ha_ref, a_ref, x_ref, l_ref, r_ref, f_ref, el_ref, er_ref,
    hm_ref, hx_ref, cw_ref, zs_ref, out_ref, kl_ref, sums, low, high
):
    half = pl.program_id(1)
    ha = ha_ref[0]
    per = rows // span

    @pl.when(jnp.logical_and(pl.program_id(0) == 0, half == 0))
    def _():
        kl_ref[...] = jnp.zeros_like(kl_ref)

    low[...] = el_ref[0].astype(F32)
    high[...] = er_ref[0].astype(F32)

    def pool(parts):
        return jnp.dot(a_ref[...], jnp.concatenate(parts, axis=0), preferred_element_type=F32)

    def local(i):
        r = half * per - 1 + i
        x = x_ref[pl.ds(pl.multiple_of(r * 112, 16), 112), :]
        face = with_corners(f_ref[0, r], low[pl.ds(r, 1), :], high[pl.ds(r, 1), :])
        sums[i] = pool([x, beside(l_ref[0, r], r_ref[0, r]), face])

    for i, side, here in ((0, half == 0, ha == 1), (per + 1, half == span - 1, ha == 0)):

        @pl.when(jnp.logical_not(side))
        def _(i=i):
            local(i)

        @pl.when(jnp.logical_and(side, here))
        def _(i=i):
            sums[i] = pool([hm_ref[...], hx_ref[0]])

        @pl.when(jnp.logical_and(side, jnp.logical_not(here)))
        def _(i=i):
            sums[i] = jnp.zeros(sums.shape[1:], F32)

    for i in range(1, per + 1):
        local(i)

    chunk = 16
    for k in range(per):
        row = ha * rows + half * per + k
        edge = jnp.logical_or(row == 0, row == grid_h - 1)
        part = jnp.where(edge, 1.0 / 2.0, 1.0 / 3.0)
        for j in range(112 // chunk):
            at = slice(j * chunk, (j + 1) * chunk)
            out = slice(k * 112 + j * chunk, k * 112 + (j + 1) * chunk)
            scale = (cw_ref[at, :] * part)[:, 0:1]
            z = (sums[k, at, :] + sums[k + 1, at, :] + sums[k + 2, at, :]) * scale
            z = z - jnp.max(z, axis=1, keepdims=True)
            e = jnp.exp2(z)
            zs = zs_ref[out, :]
            total = jnp.sum(e, axis=1, keepdims=True)
            cross = jnp.sum(e * (z - zs), axis=1, keepdims=True)
            inv = 1.0 / total
            out_ref[out, :] = (jnp.exp2(zs) - e * (2.0 * inv)).astype(BF16)
            kl_ref[at, :] += jnp.broadcast_to(cross * inv - jnp.log2(total) + 1.0, (chunk, 128))


def head_kernel(last, i_ref, f_ref, g_ref, out_ref, *acc):
    step = pl.program_id(0)
    part = lax.dot_general(f_ref[...], g_ref[...], (((0,), (0,)), ((), ())), preferred_element_type=F32)
    total = acc[0] if acc else out_ref

    @pl.when(step == 0)
    def _():
        total[...] = part

    @pl.when(jnp.logical_and(step > 0, step < last))
    def _():
        total[...] += part

    @pl.when(step == last)
    def _():
        out_ref[...] = (total[...] + part).astype(out_ref.dtype)


def back_kernel(g_ref, w_ref, out_ref):
    out_ref[...] = jnp.dot(g_ref[...], w_ref[...], preferred_element_type=F32).astype(BF16)


def local(features, teacher, head_weight):
    batch, frames, rows, columns, width = features.shape
    classes = teacher.shape[-1]
    n_wa = lax.axis_size("wa")
    grid_w = columns * n_wa
    grid_h = rows * lax.axis_size("ha")
    grid_t = frames * lax.axis_size("ta")
    ta, ha, wa = (lax.axis_index(name).astype(jnp.int32) for name in AXES)
    tokens = batch * rows * columns * frames
    group = columns * frames
    lines = batch * rows
    forward = [(i, i + 1) for i in range(n_wa - 1)]
    backward = [(i + 1, i) for i in range(n_wa - 1)]

    feat = features.transpose(0, 2, 3, 1, 4).reshape(tokens, width)
    teach5 = teacher.transpose(0, 2, 3, 1, 4)
    teach = teach5.reshape(tokens, classes)
    wt = head_weight.T

    edge_t = jnp.where(ta == 0, frames - 1, 0)
    pick = np.arange(16)[:, None] * frames
    sel = (jnp.arange(group)[None, :] == pick + edge_t).astype(BF16)
    h_edge = jnp.where(ha == 0, rows - 1, 0).reshape(1)

    steps = 4
    per = lines // steps
    whole = lambda *shape: pl.BlockSpec(shape, lambda i, h: (0,) * len(shape))
    bf = lambda *shape: jax.ShapeDtypeStruct(shape, BF16)
    first, last, row, face, edge0, edge1 = pl.pallas_call(
        functools.partial(prep_kernel, rows, columns, steps, batch),
        grid_spec=pltpu.PrefetchScalarGridSpec(
            num_scalar_prefetch=1,
            grid=(steps,),
            in_specs=[
                whole(16, group),
                pl.BlockSpec((per * group, classes), lambda i, h: (i, 0)),
                pl.BlockSpec((lines, 1, frames, classes), lambda i, h: (0, 0, 0, 0)),
                pl.BlockSpec((lines, 1, frames, classes), lambda i, h: (0, columns - 1, 0, 0)),
                pl.BlockSpec((batch, 1, columns, frames, classes), lambda i, h: (0, h[0], 0, 0, 0)),
            ],
            out_specs=[
                whole(lines, frames, classes),
                whole(lines, frames, classes),
                whole(batch * columns, frames, classes),
                whole(lines * 16, classes),
                whole(batch * 16, classes),
                whole(batch * 16, classes),
            ],
            scratch_shapes=[pltpu.VMEM((batch * 16, classes), F32)] * 2,
        ),
        out_shape=[
            bf(lines, frames, classes),
            bf(lines, frames, classes),
            bf(batch * columns, frames, classes),
            bf(lines * 16, classes),
            bf(batch * 16, classes),
            bf(batch * 16, classes),
        ],
        compiler_params=params(),
        cost_estimate=cost(10**9, 12 * 10**6),
    )(h_edge, sel, teach, *[teach5.reshape(lines, columns, frames, classes)] * 2, teach5)

    edge1 = lax.ppermute(edge1, "ta", SWAP)
    edge0 = lax.ppermute(edge0, "ta", SWAP)
    face = lax.ppermute(face, "ta", SWAP)
    left = lax.ppermute(last, "wa", forward)
    right = lax.ppermute(first, "wa", backward)
    h_main = lax.ppermute(row, "ha", SWAP)
    corner_l = lax.ppermute(edge1, "wa", forward)
    corner_r = lax.ppermute(edge0, "wa", backward)

    block = 448

    def student(start, blocks, weight, before=None):
        def of(i):
            return start + jnp.clip(i, 0, blocks - 1)

        convert = before is None
        outs = [pl.BlockSpec((block, classes), lambda i: (of(i - 1), 0))]
        shapes = [jax.ShapeDtypeStruct((tokens, classes), F32)]
        if convert:
            outs.append(pl.BlockSpec((classes, width), lambda i: (0, 0)))
            shapes.append(bf(classes, width))
        return pl.pallas_call(
            functools.partial(student_kernel, blocks, convert),
            grid=(blocks + 1,),
            in_specs=[
                pl.BlockSpec((block, width), lambda i: (of(i), 0)),
                pl.BlockSpec((classes, width), lambda i: (0, 0)),
            ] + ([] if convert else [pl.BlockSpec(memory_space=pl.ANY)]),
            out_specs=outs,
            out_shape=shapes,
            input_output_aliases={} if convert else {2: 0},
            scratch_shapes=[pltpu.VMEM((block, classes), F32)] * 2,
            compiler_params=params(),
            cost_estimate=cost(
                2 * blocks * block * width * classes, blocks * block * 6000, blocks * block * classes
            ),
        )(feat, weight, *([] if convert else [before]))

    half_a = 4
    zs, wt_bf = student(0, half_a, wt)

    left4 = left.reshape(batch, rows, frames, classes)
    right4 = right.reshape(batch, rows, frames, classes)
    face4 = face.reshape(batch, rows, 16, classes)
    low3 = corner_l.reshape(batch, 16, classes)
    high3 = corner_r.reshape(batch, 16, classes)
    at_edge = lambda n: pl.BlockSpec((batch, 1, n, classes), lambda i, h: (0, h[0], 0, 0))
    packed = pl.pallas_call(
        functools.partial(pack_kernel, batch),
        grid_spec=pltpu.PrefetchScalarGridSpec(
            num_scalar_prefetch=1,
            grid=(1,),
            in_specs=[at_edge(frames), at_edge(frames), at_edge(16), whole(batch, 16, classes), whole(batch, 16, classes)],
            out_specs=whole(batch, 32, classes),
        ),
        out_shape=bf(batch, 32, classes),
        compiler_params=params(),
        cost_estimate=cost(10**6, 10**6),
    )(h_edge, left4, right4, face4, low3, high3)
    h_ext = lax.ppermute(packed, "ha", SWAP)
    wt_bf, _ = lax.optimization_barrier((wt_bf, packed))
    (zs,) = student(half_a, tokens // block - half_a, wt_bf, zs)

    k = np.arange(144)
    kw = np.where(k < 112, k // 8, np.where(k < 120, -1, np.where(k < 128, 14, k - 128)))
    kw = np.where(k == 142, -1, np.where(k == 143, 14, kw))
    kt = np.where(k < 112, k % 8, np.where(k < 128, (k - 112) % 8, 0))
    halo = k >= 128
    kt = jnp.where(halo, jnp.where(ta == 0, frames, -1), kt)[None, :]
    kw = kw[None, :]
    w = (np.arange(group) // frames)[:, None]
    t = (np.arange(group) % frames)[:, None]
    col, kcol = wa * columns + w, wa * columns + kw
    near = (abs(w - kw) <= 1) & (abs(t - kt) <= 1)
    ok = (kcol >= 0) & (kcol < grid_w) & (clip_of(kcol) == clip_of(col))
    pool = (near & ok).astype(BF16)
    left_ok = (col > 0) & (clip_of(col - 1) == clip_of(col))
    right_ok = (col < grid_w - 1) & (clip_of(col + 1) == clip_of(col))
    frame = ta * frames + t
    count = (3.0 - (frame == 0) - (frame == grid_t - 1)) * (1.0 + left_ok + right_ok)
    scale = jnp.broadcast_to((0.5 * LOG2E) / count.astype(F32), (group, 128))

    span = 2
    big = rows // span * group
    slope, kl = pl.pallas_call(
        functools.partial(teacher_kernel, grid_h, rows, span),
        grid=(batch, span),
        in_specs=[
            pl.BlockSpec(memory_space=pltpu.SMEM),
            pl.BlockSpec((group, 144), lambda b, s: (0, 0)),
            pl.BlockSpec((rows * group, classes), lambda b, s: (b, 0)),
            pl.BlockSpec((1, rows, frames, classes), lambda b, s: (b, 0, 0, 0)),
            pl.BlockSpec((1, rows, frames, classes), lambda b, s: (b, 0, 0, 0)),
            pl.BlockSpec((1, rows, 16, classes), lambda b, s: (b, 0, 0, 0)),
            pl.BlockSpec((1, 16, classes), lambda b, s: (b, 0, 0)),
            pl.BlockSpec((1, 16, classes), lambda b, s: (b, 0, 0)),
            pl.BlockSpec((group, classes), lambda b, s: (b, 0)),
            pl.BlockSpec((1, 32, classes), lambda b, s: (b, 0, 0)),
            pl.BlockSpec((group, 128), lambda b, s: (0, 0)),
            pl.BlockSpec((big, classes), lambda b, s: (b * span + s, 0)),
        ],
        out_specs=[
            pl.BlockSpec((big, classes), lambda b, s: (b * span + s, 0)),
            pl.BlockSpec((group, 128), lambda b, s: (0, 0)),
        ],
        out_shape=[
            jax.ShapeDtypeStruct((tokens, classes), BF16),
            jax.ShapeDtypeStruct((group, 128), F32),
        ],
        scratch_shapes=[
            pltpu.VMEM((rows // span + 2, group, classes), F32),
            pltpu.VMEM((16, classes), F32),
            pltpu.VMEM((16, classes), F32),
        ],
        compiler_params=params(),
        cost_estimate=cost(4 * 10**9, 27 * 10**6, 2 * tokens * classes),
    )(
        ha.reshape(1),
        pool,
        teach,
        left4,
        right4,
        face4,
        low3,
        high3,
        h_main.reshape(batch * group, classes),
        h_ext,
        scale,
        zs,
    )

    n_dev = lax.axis_size(AXES)
    owned = width // n_dev
    side = width // 2
    deep = tokens // 2

    def head(which, dtype):
        return pl.pallas_call(
            functools.partial(head_kernel, tokens // deep - 1),
            grid_spec=pltpu.PrefetchScalarGridSpec(
                num_scalar_prefetch=1,
                grid=(tokens // deep,),
                in_specs=[
                    pl.BlockSpec((deep, side), lambda i, n: (i, n[0])),
                    pl.BlockSpec((deep, classes), lambda i, n: (i, 0)),
                ],
                out_specs=pl.BlockSpec((side, classes), lambda i, n: (0, 0)),
                scratch_shapes=[] if dtype == F32 else [pltpu.VMEM((side, classes), F32)],
            ),
            out_shape=jax.ShapeDtypeStruct((side, classes), dtype),
            compiler_params=params(),
            cost_estimate=cost(2 * tokens * side * classes, 12 * 10**6),
        )(which.reshape(1), feat, slope)

    split = lambda x: x.reshape(n_dev // 2, owned, classes)
    theirs = lax.ppermute(split(head(1 - ta, BF16)), "ta", SWAP)
    ours = split(head(ta, F32))
    both = (ours + theirs.astype(F32)).astype(BF16)
    pieces = lax.all_to_all(both, ("ha", "wa"), 0, 0, tiled=True)

    feat_grad = pl.pallas_call(
        back_kernel,
        grid=(tokens // block,),
        in_specs=[
            pl.BlockSpec((block, classes), lambda i: (i, 0)),
            pl.BlockSpec((classes, width), lambda i: (0, 0)),
        ],
        out_specs=pl.BlockSpec((block, width), lambda i: (i, 0)),
        out_shape=bf(tokens, width),
        compiler_params=params(),
        cost_estimate=cost(2 * tokens * width * classes, 15 * 10**6),
    )(slope, wt_bf)

    pieces, feat_grad = lax.optimization_barrier((pieces, feat_grad))
    feature_grad = feat_grad.reshape(batch, rows, columns, frames, width).transpose(0, 3, 1, 2, 4)
    mine = jnp.sum(pieces.astype(F32), axis=0)
    pair = jnp.stack([jnp.sum(mine * mine), jnp.sum(kl[:, 0])])
    pair = jnp.pad(pair, (0, 126)).reshape(1, 1, 128)
    pair = lax.all_to_all(jnp.broadcast_to(pair, (n_dev, 1, 128)), AXES, 0, 0, tiled=True)
    pair = jnp.sum(pair, axis=(0, 1))
    loss = pair[1] * (4.0 * LN2)
    clip = jnp.minimum(1.0, CLIP / (jnp.sqrt(pair[0]) + 1e-06))
    start = lax.axis_index(AXES) * owned
    weight_rows = lax.dynamic_slice_in_dim(head_weight, start, owned, 0)
    new_weight = weight_rows - LR * clip * mine
    return feature_grad, loss, new_weight


def solution(mesh):
    placed = P(None, "ta", "ha", "wa", None)
    return jax.shard_map(
        local,
        mesh=mesh,
        in_specs=(placed, placed, P()),
        out_specs=(placed, P(), P(AXES, None)),
        check_vma=False,
    )
```
